768 devices in a mesh: gz: 16 (over y, x_lo), gy: 48 (over z, x_hi, core).
Axes of the slice: x: 4 (x_hi: 2, x_lo: 2; x = x_hi * 2 + x_lo), y: 8, z: 12, core: 2. Of those that a mesh axis runs over, the one named last changes fastest.
Arguments:
- velocity: float32 [3, 128, 768, 768], P(None, 'gz', 'gy'), may hold values from -6 to 6
- forces: bfloat16 [24576, 3, 128], P(('gz', 'gy')), may hold values from -6 to 6
- kernels: bfloat16 [24576, 128, 256], P(('gz', 'gy')), may hold values from -0.5 to 0.5
- owners: int32 [24576, 1], P(('gz', 'gy')), may hold values from 0 to 47; in each aligned block of 32 rows (0 to 31, 32 to 63, ...) at most 2 rows name the same one
- blocks: int32 [24576], P(('gz', 'gy')), may hold values from 0 to 383
- counts: int32 [768], P(('gz', 'gy')), may hold values from 16 to 32, as said below
Outputs:
- velocity_next: float32 [3, 128, 768, 768], P(None, 'gz', 'gy')
- patch_velocity: float32 [24576, 3, 128], P(('gz', 'gy'))
The draws below stay inside these ranges and needn't reach their ends.
Inputs may be any that keep to these rules, and one draw needn't show every extreme that they name: `owners`: owners are gy indices in the holder's own row along gz; among the 32 patches of one device at most 2 share an owner, and some owner has exactly 2. `blocks`: A cell block index within the owner's part of the grid. `counts`: live patches come first in a device's slots; some device has all 32 live.
All inputs are finite; a program needn't handle non-finite values.
Results may differ from the reference program's by a relative error of at most 0.0027.
Values may be sent and summed in bfloat16 or wider, within the bound.
No kernel may reach another device: no remote copies, remote signals or barrier semaphores. Data moves between devices by JAX's collectives and lax.ppermute only.
A program may use at most 32 MiB of HBM per device.

```python
import math
import jax
import jax.numpy as jnp
import numpy as np
from jax import lax

CZ = 8
CY = 16
NX = 768
PD = 32
PTS = 128
BLK = 256
NBLK = 384
CAP = 2
NZ = 128
NY = 768
PATCHES = 24576
N_GZ = 16
N_GY = 48


def draw_counts(key, part):
    total = N_GZ * N_GY
    values = jax.random.randint(key, (total,), PD // 2, PD + 1).astype(jnp.int32)
    chosen = jax.random.randint(jax.random.fold_in(key, 7), (), 0, total).astype(jnp.int32)
    return values.at[chosen].set(PD)


def touch_ends(values, key, low, high):
    spot = [jax.random.randint(jax.random.fold_in(key, axis), (), 0, length) for axis, length in enumerate(values.shape)]
    main_axis = values.shape.index(max(values.shape))
    next_to = spot[:main_axis] + [(spot[main_axis] + 1) % values.shape[main_axis]] + spot[main_axis + 1:]
    return values.at[tuple(spot)].set(low).at[tuple(next_to)].set(high)


def shard_levels(stream_key, extent, shards, low, largest):
    gain, own = 1.0, jax.random.fold_in(stream_key, 6)
    for position, shards_of in shards:
        steps = jnp.exp(jax.random.uniform(jax.random.fold_in(own, position), (shards_of,), jnp.float32, low / len(shards), largest / len(shards)))
        gain = gain * jnp.repeat(steps, extent[position] // shards_of).reshape([-1 if axis == position else 1 for axis in range(len(extent))])
    return gain


def deal_out(own_key, own, number, rows, amount, top, bound, lean):
    order = jax.random.permutation(own_key, amount)
    crowded, usual = portions_of(amount, rows * top, bound, lean, True), portions_of(amount, rows * top, bound, lean, False)
    places = jnp.arange(amount)

    def named(lengths, offset_by):
        used = int((lengths > 0).sum())
        fixed = max(1, used // 4)
        moved = fixed + (places - fixed + offset_by * (used - fixed)) % max(1, amount - fixed)
        return jnp.zeros((amount,), jnp.int32).at[order[jnp.where(places < fixed, places, moved)]].set(jnp.asarray(lengths, jnp.int32))

    lengths = jnp.where(number % 4 == 0, named(crowded, number // 4), named(usual, number - number // 4 - 1))
    mixed = jax.random.permutation(jax.random.fold_in(own, 3), amount)
    giver, receiver = mixed[0:amount // 2 * 2:2], mixed[1:amount // 2 * 2:2]
    slack = jnp.minimum(lengths[giver] - 1, bound - lengths[receiver]) // 2
    slack = jnp.where((giver == order[0]) | (receiver == order[0]) | (lengths[receiver] == 0), 0, jnp.maximum(slack, 0))
    moved = jax.random.randint(jax.random.fold_in(own, 4), (amount // 2,), 0, 1 << 20) % (slack + 1)
    lengths = lengths.at[giver].add(-moved).at[receiver].add(moved)
    items = jnp.searchsorted(jnp.cumsum(lengths), jnp.arange(rows * top), side="right").astype(jnp.int32)
    table = items.reshape(top, rows).T
    table = table[jax.random.permutation(jax.random.fold_in(own, 1), rows)]
    offset_by = jax.random.randint(jax.random.fold_in(own, 2), (rows, 1), 0, top)
    return jnp.take_along_axis(table, (jnp.arange(top)[None, :] + offset_by) % top, axis=1)


def portions_of(number_of, total, most, slope, full):
    loads = [(1 << 20) // math.isqrt(standing ** slope) + 1 for standing in range(1, number_of + 1)]
    largest = most if full else min(most, max(-(-total // number_of), total * loads[0] // sum(loads)))
    least = 1 if total - largest >= number_of - 1 else 0
    holding, rest = [largest] + [least] * (number_of - 1), total - largest - least * (number_of - 1)
    while rest > 0:
        movable = [i for i in range(1, number_of) if holding[i] < largest] or [i for i in range(1, number_of) if holding[i] < most]
        whole, remaining = sum([loads[i] for i in movable]), rest
        for i in movable:
            addition = min(most - holding[i], max(1, remaining * loads[i] // whole), rest)
            holding[i] = holding[i] + addition
            rest = rest - addition
    return np.array(holding)


def gaussian(stream_key, shape, scale, reach, cuts=(), held_as=jnp.bfloat16):
    drawn = scale * jax.random.normal(stream_key, shape, jnp.float32)
    if cuts:
        drawn = drawn * shard_levels(stream_key, shape, cuts, -0.22, 0.18)
    return jnp.clip(drawn, -reach, reach).astype(held_as)


def setup_inputs(seed: int = 0) -> dict:
    splits = jax.random.split(jax.random.key(seed), 7)
    velocity = gaussian(splits[0], (3, NZ, NY, NX), 1.0, 6.0, ((1, 16), (2, 48)), jnp.float32)
    forces = gaussian(splits[1], (PATCHES, 3, PTS), 1.0, 6.0, ((0, 768),))
    kernels = gaussian(splits[2], (PATCHES, PTS, BLK), PTS ** -0.5, 0.5, ((0, 768),))
    owners_keys = jax.random.split(jax.random.fold_in(splits[3], 1), PATCHES // PD)
    owners_turns = jax.random.permutation(jax.random.fold_in(splits[3], 3), PATCHES // PD)
    owners = jax.vmap(lambda own, number: deal_out(jax.random.fold_in(splits[3], 2), own, number, PD, N_GY, 1, CAP, 2))(owners_keys, owners_turns).reshape((PATCHES, 1))
    blocks = touch_ends(jax.random.randint(splits[4], (PATCHES,), 0, NBLK), jax.random.fold_in(splits[4], 1), 0, NBLK - 1).astype(jnp.int32)
    counts = draw_counts(jax.random.fold_in(splits[6], 71), 0)
    return dict(velocity=velocity, forces=forces, kernels=kernels, owners=owners, blocks=blocks, counts=counts)


time_step = 0.25
viscosity = 0.5


def reference(velocity, forces, kernels, owners, blocks, counts):
    devices = N_GZ * N_GY
    xblocks = NX // BLK
    forces_dev = forces.reshape(devices, PD, 3, PTS)
    kernels_dev = kernels.reshape(devices, PD, PTS, BLK)
    live = (jnp.arange(PD, dtype=jnp.int32)[None, :] < counts[:, None]).astype(jnp.float32)

    def spread_one(items):
        force_pts, kernel, alive = items
        prod = jnp.einsum("pcq,pqb->pcb", force_pts.astype(jnp.float32), kernel.astype(jnp.float32))
        return (prod * alive[:, None, None]).astype(jnp.bfloat16)

    contribution = lax.map(spread_one, (forces_dev, kernels_dev, live)).reshape(devices * PD, 3, BLK)
    holder_row = ((jnp.arange(devices * PD, dtype=jnp.int32) // PD) // N_GY).astype(jnp.int32)
    owner_col = owners[:, 0].astype(jnp.int32)
    plane = blocks // (CY * xblocks)
    row_in = (blocks // xblocks) % CY
    xblock = blocks % xblocks
    global_id = (((holder_row * CZ + plane) * NY + owner_col * CY + row_in) * xblocks + xblock).astype(jnp.int32)
    force = jax.ops.segment_sum(contribution.astype(jnp.float32), global_id, num_segments=NZ * NY * xblocks)
    force = force.transpose(1, 0, 2).reshape(3, NZ, NY, NX)
    padded = jnp.pad(velocity, ((0, 0), (1, 1), (1, 1), (1, 1)))

    def plane_step(zidx):
        zero = jnp.int32(0)
        window = lax.dynamic_slice(padded, (zero, zidx, zero, zero), (3, 3, NY + 2, NX + 2))
        center = window[:, 1, 1:-1, 1:-1]
        x_up = window[:, 1, 1:-1, 2:]
        x_down = window[:, 1, 1:-1, :-2]
        y_up = window[:, 1, 2:, 1:-1]
        y_down = window[:, 1, :-2, 1:-1]
        z_up = window[:, 2, 1:-1, 1:-1]
        z_down = window[:, 0, 1:-1, 1:-1]
        lap = x_up + x_down + y_up + y_down + z_up + z_down - 6.0 * center
        adv = center[0:1] * (x_up - x_down) * 0.5 + center[1:2] * (y_up - y_down) * 0.5 + center[2:3] * (z_up - z_down) * 0.5
        force_plane = lax.dynamic_index_in_dim(force, zidx, 1, keepdims=False)
        return center + time_step * (viscosity * lap - adv + force_plane)

    fresh = lax.map(plane_step, jnp.arange(NZ, dtype=jnp.int32)).transpose(1, 0, 2, 3)
    cell_blocks = fresh.reshape(3, NZ * NY * xblocks, BLK)

    def sample_one(items):
        ids, kernel, alive = items
        picked = jnp.take(cell_blocks, ids, axis=1).transpose(1, 0, 2).astype(jnp.bfloat16)
        result = jnp.einsum("pcb,pqb->pcq", picked.astype(jnp.float32), kernel.astype(jnp.float32))
        return result * alive[:, None, None]

    sampled = lax.map(sample_one, (global_id.reshape(devices, PD), kernels_dev, live))
    return fresh, sampled.reshape(devices * PD, 3, PTS)
```

```python
import jax
import jax.numpy as jnp
from jax import lax
from jax.experimental import pallas as pl
from jax.experimental.pallas import tpu as pltpu
from jax.sharding import PartitionSpec as P

time_step = 0.25
viscosity = 0.5
F32 = jnp.float32
BF16 = jnp.bfloat16
LANES = 128
ROWS = 8
VMEM = pltpu.VMEM
TRANSPOSED = (((0,), (0,)), ((), ()))
NT = (((1,), (1,)), ((), ()))


def iota(shape, axis):
    return lax.broadcasted_iota(jnp.int32, shape, axis)


def column(row):
    n = row.shape[1]
    same = iota((n, n), 0) == iota((n, n), 1)
    return jnp.sum(jnp.where(same, row, 0), axis=1, keepdims=True)


def dot(a, b, dims=(((1,), (0,)), ((), ()))):
    return lax.dot_general(a, b, dims, preferred_element_type=F32)


def spread(xblocks, counts, forces, kernels, owners, blocks, send, select, product):
    slots = kernels.shape[0]
    comps = forces.shape[0]
    cells = kernels.shape[2]
    room = send.shape[0]
    wide = select.shape[1]
    tall = slots * ROWS
    owner_row = owners[...]
    owner = column(owner_row)
    block = column(blocks[...])
    here = iota((slots, slots), 0)
    there = iota((slots, slots), 1)
    earlier = (owner == owner_row) & (there < here)
    rank = jnp.sum(earlier.astype(jnp.int32), axis=1, keepdims=True)
    live = iota((slots, 1), 0) < counts[0]
    slot = jnp.where(live, owner * 2 + rank, -1)
    choose = (slot == iota((slots, wide), 1)).astype(F32).astype(BF16)
    grow = (iota((tall, slots), 0) // ROWS == iota((tall, slots), 1)).astype(F32).astype(BF16)
    tall_choose = dot(grow, choose)
    select[...] = tall_choose.astype(BF16)
    grow_t = (iota((slots, tall), 1) // ROWS == iota((slots, tall), 0)).astype(F32).astype(BF16)
    wide_choose = dot(choose, grow_t, TRANSPOSED)
    flat = forces[...].reshape(comps * slots, forces.shape[2])
    r = iota((tall, comps * slots), 0)
    s = iota((tall, comps * slots), 1)
    order = ((r % ROWS) * slots + r // ROWS == s).astype(F32).astype(BF16)
    ordered = dot(order, flat)
    for p in range(slots):
        one = ordered[p * ROWS:(p + 1) * ROWS].astype(BF16)
        product[p * ROWS:(p + 1) * ROWS, :] = dot(one, kernels[p])
    made = product[...].astype(BF16)
    lane = iota(wide_choose.shape, 1) % ROWS
    for c in range(comps):
        pick = jnp.where(lane == c, wide_choose, 0.0).astype(BF16)
        send[:, c * cells:(c + 1) * cells] = dot(pick, made)[:room].astype(BF16)
    where = iota((slots, LANES), 1)
    words = jnp.where(where == 0, block // xblocks, jnp.where(where == 1, block % xblocks, jnp.where(where == 2, 1, 0)))
    tags = dot(choose, words.astype(F32).astype(BF16), TRANSPOSED)
    send[:, comps * cells:] = tags[:room].astype(BF16)


def faces(planes, velocity, z_low, z_high, y_low, y_high):
    comps, height, _ = velocity.shape
    rows = height // planes
    for c in range(comps):
        z_low[c] = velocity[c, :rows, :].astype(BF16)
        z_high[c] = velocity[c, height - rows:, :].astype(BF16)
        for out, row in ((y_low, 0), (y_high, rows - 1)):
            picked = [velocity[c, k * rows + row:k * rows + row + 1, :] for k in range(planes)]
            out[c] = jnp.concatenate(picked, axis=0).astype(BF16)


def stencil(planes, velocity, below, above, left, right, base):
    comps, height, xcells = velocity.shape
    rows = height // planes
    x = iota((rows, xcells), 1)
    y = iota((rows, xcells), 0)
    for k in range(planes):
        span = slice(k * rows, (k + 1) * rows)
        center = [velocity[c, span, :] for c in range(comps)]
        for c in range(comps):
            v = center[c]
            x_up = jnp.where(x == xcells - 1, 0.0, pltpu.roll(v, xcells - 1, 1))
            x_down = jnp.where(x == 0, 0.0, pltpu.roll(v, 1, 1))
            y_up = jnp.where(y == rows - 1, right[c, k:k + 1, :].astype(F32), pltpu.roll(v, rows - 1, 0))
            y_down = jnp.where(y == 0, left[c, k:k + 1, :].astype(F32), pltpu.roll(v, 1, 0))
            z_up = velocity[c, (k + 1) * rows:(k + 2) * rows, :] if k + 1 < planes else above[c].astype(F32)
            z_down = velocity[c, (k - 1) * rows:k * rows, :] if k > 0 else below[c].astype(F32)
            lap = x_up + x_down + y_up + y_down + z_up + z_down - 6.0 * v
            adv = (center[0] * (x_up - x_down) + center[1] * (y_up - y_down) + center[2] * (z_up - z_down)) * 0.5
            base[c, span, :] = v + time_step * (viscosity * lap - adv)


def exchange(cells, got, base, fresh, send):
    comps, height, xcells = base.shape
    room = got.shape[0]
    xblocks = xcells // cells
    tags = got[:, comps * cells:].astype(F32)
    row, xb, valid = tags[:, 0:1], tags[:, 1:2], tags[:, 2:3]
    at = iota((room, height), 1).astype(F32)
    match = (row == at) & (valid == 1.0)
    picks = [jnp.where(match & (xb == float(b)), 1.0, 0.0) for b in range(xblocks)]
    narrow = [p.astype(BF16) for p in picks]
    turned = [p.T.astype(BF16) for p in picks]
    for c in range(comps):
        block = got[:, c * cells:(c + 1) * cells]
        total = None
        for b in range(xblocks):
            lanes = slice(b * cells, (b + 1) * cells)
            new = base[c, :, lanes] + time_step * dot(turned[b], block)
            fresh[c, :, lanes] = new
            part = dot(narrow[b], new.astype(BF16))
            total = part if total is None else total + part
        send[:, c * cells:(c + 1) * cells] = total.astype(BF16)


def sample(back, select, kernels, out, result):
    slots = kernels.shape[0]
    cells = kernels.shape[2]
    comps = out.shape[0]
    room = back.shape[0]
    chosen = select[:, :room].astype(F32)
    row = iota(chosen.shape, 0) % ROWS
    total = None
    for c in range(comps):
        pick = jnp.where(row == c, chosen, 0.0).astype(BF16)
        part = dot(pick, back[:, c * cells:(c + 1) * cells])
        total = part if total is None else total + part
    for p in range(slots):
        one = total[p * ROWS:(p + 1) * ROWS].astype(BF16)
        result[p * ROWS:(p + 1) * ROWS, :] = dot(one, kernels[p], NT)
    for c in range(comps):
        out[c] = result[pl.ds(c, slots, stride=ROWS), :]


def call(body, outs, scratch, ins):
    return pl.pallas_call(
        body,
        out_shape=outs,
        in_specs=ins,
        out_specs=[pl.BlockSpec(memory_space=VMEM)] * len(outs),
        scratch_shapes=scratch,
    )


def local(velocity, forces, kernels, owners, blocks, counts):
    width_gy = lax.axis_size("gy")
    width_gz = lax.axis_size("gz")
    slots, comps, points = forces.shape
    cells = kernels.shape[2]
    planes, rows, xcells = velocity.shape[1:]
    xblocks = xcells // cells
    room = width_gy * 2
    wide = -(-room // LANES) * LANES
    payload = comps * cells
    S = jax.ShapeDtypeStruct
    vmem = pl.BlockSpec(memory_space=VMEM)
    smem = pl.BlockSpec(memory_space=pltpu.SMEM)
    grid = velocity.reshape(comps, planes * rows, xcells)

    send, select = call(
        lambda *refs: spread(xblocks, *refs),
        [S((room, payload + LANES), BF16), S((slots * ROWS, wide), BF16)],
        [pltpu.VMEM((slots * ROWS, cells), F32)],
        [smem, vmem, vmem, vmem, vmem],
    )(counts, forces.transpose(1, 0, 2), kernels, owners.reshape(1, slots), blocks.reshape(1, slots))
    got = lax.all_to_all(send.reshape(width_gy, 2, payload + LANES), "gy", split_axis=0, concat_axis=0, tiled=True)
    got = got.reshape(room, payload + LANES)

    z_low, z_high, y_low, y_high = call(
        lambda *refs: faces(planes, *refs),
        [S((comps, rows, xcells), BF16)] * 2 + [S((comps, planes, xcells), BF16)] * 2,
        [],
        [vmem],
    )(grid)
    up_gz = [(i, i + 1) for i in range(width_gz - 1)]
    up_gy = [(i, i + 1) for i in range(width_gy - 1)]
    below = lax.ppermute(z_high, "gz", up_gz)
    above = lax.ppermute(z_low, "gz", [(b, a) for a, b in up_gz])
    left = lax.ppermute(y_high, "gy", up_gy)
    right = lax.ppermute(y_low, "gy", [(b, a) for a, b in up_gy])
    (base,) = call(
        lambda *refs: stencil(planes, *refs),
        [S(grid.shape, F32)],
        [],
        [vmem] * 5,
    )(grid, below, above, left, right)

    fresh, picked = call(
        lambda *refs: exchange(cells, *refs),
        [S(grid.shape, F32), S((room, payload), BF16)],
        [],
        [vmem] * 2,
    )(got, base)
    back = lax.all_to_all(picked.reshape(width_gy, 2, payload), "gy", split_axis=0, concat_axis=0, tiled=True)

    (out,) = call(
        sample,
        [S((comps, slots, points), F32)],
        [pltpu.VMEM((slots * ROWS, points), F32)],
        [vmem] * 3,
    )(back.reshape(room, payload), select, kernels)
    return fresh.reshape(velocity.shape), out.transpose(1, 0, 2)


def solution(mesh):
    return jax.shard_map(
        local,
        mesh=mesh,
        in_specs=(
            P(None, "gz", "gy", None),
            P(("gz", "gy"), None, None),
            P(("gz", "gy"), None, None),
            P(("gz", "gy"), None),
            P(("gz", "gy")),
            P(("gz", "gy")),
        ),
        out_specs=(P(None, "gz", "gy", None), P(("gz", "gy"), None, None)),
        check_vma=False,
    )
```

```python
import jax
import jax.numpy as jnp
from jax import lax
from jax.experimental import pallas as pl
from jax.experimental.pallas import tpu as pltpu
from jax.sharding import PartitionSpec as P


time_step = 0.25
viscosity = 0.5
F32 = jnp.float32
BF16 = jnp.bfloat16
LANES = 128
ROWS = 8
VMEM = pltpu.VMEM
TRANSPOSED = (((0,), (0,)), ((), ()))
NT = (((1,), (1,)), ((), ()))


def iota(shape, axis):
    return lax.broadcasted_iota(jnp.int32, shape, axis)


def column(row):
    n = row.shape[1]
    same = iota((n, n), 0) == iota((n, n), 1)
    return jnp.sum(jnp.where(same, row, 0), axis=1, keepdims=True)


def dot(a, b, dims=(((1,), (0,)), ((), ()))):
    return lax.dot_general(a, b, dims, preferred_element_type=F32)


def spread(xblocks, counts, *refs):
    sources, (send, select, product, kernels), small, arrived = refs[:4], refs[4:8], refs[8:11], refs[11]
    forces, owners, blocks = small
    slots = kernels.shape[0]
    parts = arrived.shape[0] - len(small)
    tables = []
    for i, (source, target) in enumerate(zip(sources[1:], small)):
        tables.append(pltpu.make_async_copy(source, target, arrived.at[parts + i]))
        tables[-1].start()
    source = sources[0]
    each = slots // parts
    copies = []
    for i in range(parts):
        span = pl.ds(i * each, each)
        copies.append(pltpu.make_async_copy(source.at[span], kernels.at[span], arrived.at[i]))
        copies[-1].start()
    comps = forces.shape[0]
    cells = kernels.shape[2]
    room = send.shape[0]
    wide = select.shape[1]
    tall = slots * ROWS
    for copy in tables:
        copy.wait()
    owner_row = owners[...]
    owner = column(owner_row)
    block = column(blocks[...])
    here = iota((slots, slots), 0)
    there = iota((slots, slots), 1)
    earlier = (owner == owner_row) & (there < here)
    rank = jnp.sum(earlier.astype(jnp.int32), axis=1, keepdims=True)
    live = iota((slots, 1), 0) < counts[0]
    slot = jnp.where(live, owner * 2 + rank, -1)
    choose = (slot == iota((slots, wide), 1)).astype(F32).astype(BF16)
    grow = (iota((tall, slots), 0) // ROWS == iota((tall, slots), 1)).astype(F32).astype(BF16)
    tall_choose = dot(grow, choose)
    select[...] = tall_choose.astype(BF16)
    grow_t = (iota((slots, tall), 1) // ROWS == iota((slots, tall), 0)).astype(F32).astype(BF16)
    wide_choose = dot(choose, grow_t, TRANSPOSED)
    flat = forces[...].reshape(comps * slots, forces.shape[2])
    r = iota((tall, comps * slots), 0)
    s = iota((tall, comps * slots), 1)
    order = ((r % ROWS) * slots + r // ROWS == s).astype(F32).astype(BF16)
    ordered = dot(order, flat)
    for p in range(slots):
        if p % each == 0:
            copies[p // each].wait()
        one = ordered[p * ROWS:(p + 1) * ROWS].astype(BF16)
        product[p * ROWS:(p + 1) * ROWS, :] = dot(one, kernels[p])
    made = product[...].astype(BF16)
    lane = iota(wide_choose.shape, 1) % ROWS
    for c in range(comps):
        pick = jnp.where(lane == c, wide_choose, 0.0).astype(BF16)
        send[:, c * cells:(c + 1) * cells] = dot(pick, made)[:room].astype(BF16)
    where = iota((slots, LANES), 1)
    words = jnp.where(where == 0, block // xblocks, jnp.where(where == 1, block % xblocks, jnp.where(where == 2, 1, 0)))
    tags = dot(choose, words.astype(F32).astype(BF16), TRANSPOSED)
    send[:, comps * cells:] = tags[:room].astype(BF16)


def even(axis):
    return lax.axis_index(axis) % 2 == 0


def faces(planes, velocity, z_near, z_far, y_near, y_far):
    comps, height, _ = velocity.shape
    rows = height // planes
    z_even, y_even = even("gz"), even("gy")
    for c in range(comps):
        low, high = velocity[c, :rows, :].astype(BF16), velocity[c, height - rows:, :].astype(BF16)
        z_near[c] = jnp.where(z_even, high, low)
        z_far[c] = jnp.where(z_even, low, high)
        low, high = [jnp.concatenate([velocity[c, k * rows + row:k * rows + row + 1, :] for k in range(planes)], axis=0).astype(BF16) for row in (0, rows - 1)]
        y_near[c] = jnp.where(y_even, high, low)
        y_far[c] = jnp.where(y_even, low, high)


def stencil(planes, velocity, near_side, far_side, base):
    comps, height, xcells = velocity.shape
    rows = height // planes
    y_even = even("gy")
    left = [jnp.where(y_even, far_side[c].astype(F32), near_side[c].astype(F32)) for c in range(comps)]
    right = [jnp.where(y_even, near_side[c].astype(F32), far_side[c].astype(F32)) for c in range(comps)]
    x = iota((rows, xcells), 1)
    y = iota((rows, xcells), 0)
    for k in range(planes):
        span = slice(k * rows, (k + 1) * rows)
        center = [velocity[c, span, :] for c in range(comps)]
        for c in range(comps):
            v = center[c]
            x_up = jnp.where(x == xcells - 1, 0.0, pltpu.roll(v, xcells - 1, 1))
            x_down = jnp.where(x == 0, 0.0, pltpu.roll(v, 1, 1))
            y_up = jnp.where(y == rows - 1, right[c][k:k + 1, :], pltpu.roll(v, rows - 1, 0))
            y_down = jnp.where(y == 0, left[c][k:k + 1, :], pltpu.roll(v, 1, 0))
            z_up = velocity[c, (k + 1) * rows:(k + 2) * rows, :] if k + 1 < planes else 0.0
            z_down = velocity[c, (k - 1) * rows:k * rows, :] if k > 0 else 0.0
            lap = x_up + x_down + y_up + y_down + z_up + z_down - 6.0 * v
            adv = (center[0] * (x_up - x_down) + center[1] * (y_up - y_down) + center[2] * (z_up - z_down)) * 0.5
            base[c, span, :] = v + time_step * (viscosity * lap - adv)


def exchange(cells, rows, got, base, velocity, near_side, far_side, fresh, send):
    comps, height, xcells = base.shape
    z_even = even("gz")
    below = [jnp.where(z_even, far_side[c].astype(F32), near_side[c].astype(F32)) for c in range(comps)]
    above = [jnp.where(z_even, near_side[c].astype(F32), far_side[c].astype(F32)) for c in range(comps)]
    room = got.shape[0]
    xblocks = xcells // cells
    tags = got[:, comps * cells:].astype(F32)
    row, xb, valid = tags[:, 0:1], tags[:, 1:2], tags[:, 2:3]
    at = iota((room, height), 1).astype(F32)
    match = (row == at) & (valid == 1.0)
    picks = [jnp.where(match & (xb == float(b)), 1.0, 0.0) for b in range(xblocks)]
    narrow = [p.astype(BF16) for p in picks]
    turned = [p.T.astype(BF16) for p in picks]
    for c in range(comps):
        block = got[:, c * cells:(c + 1) * cells]
        total = None
        for b in range(xblocks):
            lanes = slice(b * cells, (b + 1) * cells)
            lift = velocity[comps - 1, :rows, lanes] * (0.5 * time_step) + viscosity * time_step
            sink = viscosity * time_step - velocity[comps - 1, height - rows:, lanes] * (0.5 * time_step)
            low = below[c][:, lanes] * lift
            high = above[c][:, lanes] * sink
            flow = jnp.concatenate([low + base[c, :rows, lanes], base[c, rows:height - rows, lanes], high + base[c, height - rows:, lanes]], axis=0)
            new = flow + time_step * dot(turned[b], block)
            fresh[c, :, lanes] = new
            part = dot(narrow[b], new.astype(BF16))
            total = part if total is None else total + part
        send[:, c * cells:(c + 1) * cells] = total.astype(BF16)


def sample(back, select, kernels, out, result):
    slots = kernels.shape[0]
    cells = kernels.shape[2]
    comps = out.shape[0]
    room = back.shape[0]
    chosen = select[:, :room].astype(F32)
    row = iota(chosen.shape, 0) % ROWS
    total = None
    for c in range(comps):
        pick = jnp.where(row == c, chosen, 0.0).astype(BF16)
        part = dot(pick, back[:, c * cells:(c + 1) * cells])
        total = part if total is None else total + part
    for p in range(slots):
        one = total[p * ROWS:(p + 1) * ROWS].astype(BF16)
        result[p * ROWS:(p + 1) * ROWS, :] = dot(one, kernels[p], NT)
    for c in range(comps):
        out[c] = result[pl.ds(c, slots, stride=ROWS), :]


def call(body, outs, scratch, ins, aliases={}):
    return pl.pallas_call(
        body,
        out_shape=outs,
        in_specs=ins,
        out_specs=[pl.BlockSpec(memory_space=VMEM)] * len(outs),
        scratch_shapes=scratch,
        input_output_aliases=aliases,
        compiler_params=pltpu.CompilerParams(vmem_limit_bytes=16 * 1024 * 1024),
    )


def pairs(count, first):
    low = range(first, count - 1, 2)
    return [(i, i + 1) for i in low] + [(i + 1, i) for i in low]


def near(x):
    return pltpu.with_memory_space_constraint(x, VMEM)


def step(velocity, forces, kernels, owners, blocks, counts):
    width_gy = lax.axis_size("gy")
    width_gz = lax.axis_size("gz")
    slots, comps, points = forces.shape
    cells = kernels.shape[2]
    planes, rows, xcells = velocity.shape[1:]
    xblocks = xcells // cells
    room = width_gy * 2
    wide = -(-room // LANES) * LANES
    payload = comps * cells
    parts = 4
    S = VMEM
    vmem = pl.BlockSpec(memory_space=VMEM)
    smem = pl.BlockSpec(memory_space=pltpu.SMEM)
    far = pl.BlockSpec(memory_space=pltpu.HBM)
    grid = near(velocity.reshape(comps, planes * rows, xcells))

    send, select = call(
        lambda *refs: spread(xblocks, *refs),
        [S((room, payload + LANES), BF16), S((slots * ROWS, wide), BF16)],
        [VMEM((slots * ROWS, cells), F32), VMEM(kernels.shape, BF16), VMEM((comps, slots, points), BF16), VMEM((1, slots), jnp.int32), VMEM((1, slots), jnp.int32), pltpu.SemaphoreType.DMA((parts + 3,))],
        [smem] + [far] * 4,
    )(counts, *[pltpu.with_memory_space_constraint(x, pltpu.HBM) for x in (kernels, forces.transpose(1, 0, 2), owners.reshape(1, slots), blocks.reshape(1, slots))])
    got = lax.all_to_all(send.reshape(width_gy, 2, payload + LANES), "gy", split_axis=0, concat_axis=0, tiled=True)
    got = got.reshape(room, payload + LANES)

    z_near, z_far, y_near, y_far = call(
        lambda *refs: faces(planes, *refs),
        [S((comps, rows, xcells), BF16)] * 2 + [S((comps, planes, xcells), BF16)] * 2,
        [],
        [vmem],
    )(grid)
    y_near = lax.ppermute(y_near, "gy", pairs(width_gy, 0))
    y_far = lax.ppermute(y_far, "gy", pairs(width_gy, 1))
    z_near = lax.ppermute(z_near, "gz", pairs(width_gz, 0))
    z_far = lax.ppermute(z_far, "gz", pairs(width_gz, 1))
    (base,) = call(
        lambda *refs: stencil(planes, *refs),
        [S(grid.shape, F32)],
        [],
        [vmem] * 3,
    )(grid, near(y_near), near(y_far))

    fresh, picked = call(
        lambda *refs: exchange(cells, rows, *refs),
        [S(grid.shape, F32), S((room, payload), BF16)],
        [],
        [vmem] * 5,
        {1: 0},
    )(near(got), near(base), grid, near(z_near), near(z_far))
    back = lax.all_to_all(picked.reshape(width_gy, 2, payload), "gy", split_axis=0, concat_axis=0, tiled=True)

    (out,) = call(
        sample,
        [jax.ShapeDtypeStruct((comps, slots, points), F32)],
        [VMEM((slots * ROWS, points), F32)],
        [vmem] * 3,
    )(near(back.reshape(room, payload)), near(select), near(kernels))
    return fresh.reshape(velocity.shape), out.transpose(1, 0, 2)


def solution(mesh):
    return jax.shard_map(
        step,
        mesh=mesh,
        in_specs=(
            P(None, "gz", "gy", None),
            P(("gz", "gy"), None, None),
            P(("gz", "gy"), None, None),
            P(("gz", "gy"), None),
            P(("gz", "gy")),
            P(("gz", "gy")),
        ),
        out_specs=(P(None, "gz", "gy", None), P(("gz", "gy"), None, None)),
        check_vma=False,
    )
```

```python
import jax
import jax.numpy as jnp
from jax import lax
from jax.experimental import pallas as pl
from jax.experimental.pallas import tpu as pltpu
from jax.sharding import PartitionSpec as P


time_step = 0.25
viscosity = 0.5
F32 = jnp.float32
BF16 = jnp.bfloat16
LANES = 128
ROWS = 8
VMEM = pltpu.VMEM
TRANSPOSED = (((0,), (0,)), ((), ()))
NT = (((1,), (1,)), ((), ()))


def iota(shape, axis):
    return lax.broadcasted_iota(jnp.int32, shape, axis)


def column(row):
    n = row.shape[1]
    same = iota((n, n), 0) == iota((n, n), 1)
    return jnp.sum(jnp.where(same, row, 0), axis=1, keepdims=True)


def dot(a, b, dims=(((1,), (0,)), ((), ()))):
    return lax.dot_general(a, b, dims, preferred_element_type=F32)


def spread(xblocks, counts, *refs):
    sources, (send, select, product, kernels), small, arrived = refs[:4], refs[4:8], refs[8:11], refs[11]
    forces, owners, blocks = small
    slots = kernels.shape[0]
    parts = arrived.shape[0] - len(small)
    tables = []
    for i, (source, target) in enumerate(zip(sources[1:], small)):
        tables.append(pltpu.make_async_copy(source, target, arrived.at[parts + i]))
        tables[-1].start()
    source = sources[0]
    each = slots // parts
    copies = []
    for i in range(parts):
        span = pl.ds(i * each, each)
        copies.append(pltpu.make_async_copy(source.at[span], kernels.at[span], arrived.at[i]))
        copies[-1].start()
    comps = forces.shape[0]
    cells = kernels.shape[2]
    room = send.shape[0] * send.shape[1]
    wide = select.shape[1]
    tall = slots * ROWS
    for copy in tables:
        copy.wait()
    owner_row = owners[...]
    owner = column(owner_row)
    block = column(blocks[...])
    here = iota((slots, slots), 0)
    there = iota((slots, slots), 1)
    earlier = (owner == owner_row) & (there < here)
    rank = jnp.sum(earlier.astype(jnp.int32), axis=1, keepdims=True)
    live = iota((slots, 1), 0) < counts[0]
    slot = jnp.where(live, owner * 2 + rank, -1)
    choose = (slot == iota((slots, wide), 1)).astype(F32).astype(BF16)
    grow = (iota((tall, slots), 0) // ROWS == iota((tall, slots), 1)).astype(F32).astype(BF16)
    tall_choose = dot(grow, choose)
    select[...] = tall_choose.astype(BF16)
    grow_t = (iota((slots, tall), 1) // ROWS == iota((slots, tall), 0)).astype(F32).astype(BF16)
    wide_choose = dot(choose, grow_t, TRANSPOSED)
    flat = forces[...].reshape(comps * slots, forces.shape[2])
    r = iota((tall, comps * slots), 0)
    s = iota((tall, comps * slots), 1)
    order = ((r % ROWS) * slots + r // ROWS == s).astype(F32).astype(BF16)
    ordered = dot(order, flat)
    for p in range(slots):
        if p % each == 0:
            copies[p // each].wait()
        one = ordered[p * ROWS:(p + 1) * ROWS].astype(BF16)
        product[p * ROWS:(p + 1) * ROWS, :] = dot(one, kernels[p])
    made = product[...].astype(BF16)
    lane = iota(wide_choose.shape, 1) % ROWS
    for c in range(comps):
        pick = jnp.where(lane == c, wide_choose, 0.0).astype(BF16)
        send[:, :, c * cells:(c + 1) * cells] = dot(pick, made)[:room].reshape(room // 2, 2, cells).astype(BF16)
    where = iota((slots, LANES), 1)
    words = jnp.where(where == 0, block // xblocks, jnp.where(where == 1, block % xblocks, jnp.where(where == 2, 1, 0)))
    tags = dot(choose, words.astype(F32).astype(BF16), TRANSPOSED)
    send[:, :, comps * cells:] = tags[:room].reshape(room // 2, 2, LANES).astype(BF16)


def even(axis):
    return lax.axis_index(axis) % 2 == 0


def faces(planes, velocity, z_near, z_far, y_near, y_far, lifts):
    comps, height, _ = velocity.shape
    rows = height // planes
    z_even, y_even = even("gz"), even("gy")
    for c in range(comps):
        low, high = velocity[c, :rows, :].astype(BF16), velocity[c, height - rows:, :].astype(BF16)
        z_near[c] = jnp.where(z_even, high, low)
        z_far[c] = jnp.where(z_even, low, high)
        first, last = [jnp.concatenate([velocity[c, k * rows + row:k * rows + row + 1, :] for k in range(planes)], axis=0) for row in (0, rows - 1)]
        if c == 1:
            lifts[0] = viscosity + 0.5 * first
            lifts[1] = viscosity - 0.5 * last
        low, high = first.astype(BF16), last.astype(BF16)
        y_near[c] = jnp.where(y_even, high, low)
        y_far[c] = jnp.where(y_even, low, high)


def stencil(planes, velocity, base):
    comps, height, xcells = velocity.shape
    rows = height // planes
    x = iota((rows, xcells), 1)
    y = iota((rows, xcells), 0)
    for k in range(planes):
        span = slice(k * rows, (k + 1) * rows)
        center = [velocity[c, span, :] for c in range(comps)]
        for c in range(comps):
            v = center[c]
            x_up = jnp.where(x == xcells - 1, 0.0, pltpu.roll(v, xcells - 1, 1))
            x_down = jnp.where(x == 0, 0.0, pltpu.roll(v, 1, 1))
            y_up = jnp.where(y == rows - 1, 0.0, pltpu.roll(v, rows - 1, 0))
            y_down = jnp.where(y == 0, 0.0, pltpu.roll(v, 1, 0))
            z_up = velocity[c, (k + 1) * rows:(k + 2) * rows, :] if k + 1 < planes else 0.0
            z_down = velocity[c, (k - 1) * rows:k * rows, :] if k > 0 else 0.0
            lap = x_up + x_down + y_up + y_down + z_up + z_down - 6.0 * v
            adv = (center[0] * (x_up - x_down) + center[1] * (y_up - y_down) + center[2] * (z_up - z_down)) * 0.5
            base[c, span, :] = v + time_step * (viscosity * lap - adv)


def exchange(cells, planes, got, base, velocity, lifts, y_near, y_far, z_near, z_far, fresh, send):
    comps, height, xcells = base.shape
    rows = height // planes
    room = got.shape[0]
    xblocks = xcells // cells
    y_even, z_even = even("gy"), even("gz")
    tags = got[:, comps * cells:].astype(F32)
    row, xb, valid = tags[:, 0:1], tags[:, 1:2], tags[:, 2:3]
    at = iota((room, height), 1).astype(F32)
    match = (row == at) & (valid == 1.0)
    picks = [jnp.where(match & (xb == float(b)), 1.0, 0.0) for b in range(xblocks)]
    narrow = [p.astype(BF16) for p in picks]
    edge = iota((4 * planes, height), 0) % (2 * planes)
    spot = (edge % planes) * rows + jnp.where(edge >= planes, rows - 1, 0)
    edges = jnp.where(iota((4 * planes, height), 1) == spot, 1.0, 0.0)
    turned = [jnp.concatenate([p, edges], axis=0).T.astype(BF16) for p in picks]
    lift = velocity[comps - 1, :rows, :] * (0.5 * time_step) + viscosity * time_step
    sink = viscosity * time_step - velocity[comps - 1, height - rows:, :] * (0.5 * time_step)
    for c in range(comps):
        one, two = z_near[c].astype(F32), z_far[c].astype(F32)
        low = jnp.where(z_even, two, one) * lift
        high = jnp.where(z_even, one, two) * sink
        one, two = y_near[c].astype(F32), y_far[c].astype(F32)
        sides = jnp.concatenate([jnp.where(y_even, two, one) * lifts[0], jnp.where(y_even, one, two) * lifts[1]], axis=0)
        coarse = sides.astype(BF16)
        fine = (sides - coarse.astype(F32)).astype(BF16)
        total = None
        for b in range(xblocks):
            lanes = slice(b * cells, (b + 1) * cells)
            block = jnp.concatenate([got[:, c * cells:(c + 1) * cells], coarse[:, lanes], fine[:, lanes]], axis=0)
            flow = jnp.concatenate([low[:, lanes] + base[c, :rows, lanes], base[c, rows:height - rows, lanes], high[:, lanes] + base[c, height - rows:, lanes]], axis=0)
            new = flow + time_step * dot(turned[b], block)
            fresh[c, :, lanes] = new
            part = dot(narrow[b], new.astype(BF16))
            total = part if total is None else total + part
        send[:, :, c * cells:(c + 1) * cells] = total.reshape(send.shape[0], 2, cells).astype(BF16)


def sample(back, select, kernels, out, result):
    slots = kernels.shape[0]
    cells = kernels.shape[2]
    comps = out.shape[0]
    room = back.shape[0]
    chosen = select[:, :room].astype(F32)
    row = iota(chosen.shape, 0) % ROWS
    total = None
    for c in range(comps):
        pick = jnp.where(row == c, chosen, 0.0).astype(BF16)
        part = dot(pick, back[:, c * cells:(c + 1) * cells])
        total = part if total is None else total + part
    for p in range(slots):
        one = total[p * ROWS:(p + 1) * ROWS].astype(BF16)
        result[p * ROWS:(p + 1) * ROWS, :] = dot(one, kernels[p], NT)
    for c in range(comps):
        out[c] = result[pl.ds(c, slots, stride=ROWS), :]


def call(body, outs, scratch, ins, aliases={}):
    return pl.pallas_call(
        body,
        out_shape=outs,
        in_specs=ins,
        out_specs=[pl.BlockSpec(memory_space=VMEM)] * len(outs),
        scratch_shapes=scratch,
        input_output_aliases=aliases,
        compiler_params=pltpu.CompilerParams(vmem_limit_bytes=16 * 1024 * 1024),
    )


def pairs(count, first):
    low = range(first, count - 1, 2)
    return [(i, i + 1) for i in low] + [(i + 1, i) for i in low]


def near(x):
    return pltpu.with_memory_space_constraint(x, VMEM)


def step(velocity, forces, kernels, owners, blocks, counts):
    width_gy = lax.axis_size("gy")
    width_gz = lax.axis_size("gz")
    slots, comps, points = forces.shape
    cells = kernels.shape[2]
    planes, rows, xcells = velocity.shape[1:]
    xblocks = xcells // cells
    room = width_gy * 2
    wide = -(-room // LANES) * LANES
    payload = comps * cells
    parts = 4
    S = VMEM
    vmem = pl.BlockSpec(memory_space=VMEM)
    far = pl.BlockSpec(memory_space=pltpu.HBM)
    grid = near(velocity.reshape(comps, planes * rows, xcells))

    send, select = call(
        lambda *refs: spread(xblocks, *refs),
        [S((width_gy, 2, payload + LANES), BF16), S((slots * ROWS, wide), BF16)],
        [VMEM((slots * ROWS, cells), F32), VMEM(kernels.shape, BF16), VMEM((comps, slots, points), BF16), VMEM((1, slots), jnp.int32), VMEM((1, slots), jnp.int32), pltpu.SemaphoreType.DMA((parts + 3,))],
        [pl.BlockSpec(memory_space=pltpu.SMEM)] + [far] * 4,
    )(counts, *[pltpu.with_memory_space_constraint(x, pltpu.HBM) for x in (kernels, forces.transpose(1, 0, 2), owners.reshape(1, slots), blocks.reshape(1, slots))])
    got = lax.all_to_all(send, "gy", split_axis=0, concat_axis=0, tiled=True)
    got = got.reshape(room, payload + LANES)

    z_near, z_far, y_near, y_far, lifts = call(
        lambda *refs: faces(planes, *refs),
        [S((comps, rows, xcells), BF16)] * 2 + [S((comps, planes, xcells), BF16)] * 2 + [S((2, planes, xcells), F32)],
        [],
        [vmem],
    )(grid)
    y_near = lax.ppermute(y_near, "gy", pairs(width_gy, 0))
    y_far = lax.ppermute(y_far, "gy", pairs(width_gy, 1))
    z_near = lax.ppermute(z_near, "gz", pairs(width_gz, 0))
    z_far = lax.ppermute(z_far, "gz", pairs(width_gz, 1))
    (base,) = call(
        lambda *refs: stencil(planes, *refs),
        [S(grid.shape, F32)],
        [],
        [vmem],
    )(grid)

    fresh, picked = call(
        lambda *refs: exchange(cells, planes, *refs),
        [S(grid.shape, F32), S((width_gy, 2, payload), BF16)],
        [],
        [vmem] * 8,
        {1: 0},
    )(near(got), near(base), grid, near(lifts), near(y_near), near(y_far), near(z_near), near(z_far))
    back = lax.all_to_all(picked, "gy", split_axis=0, concat_axis=0, tiled=True)

    (out,) = call(
        sample,
        [jax.ShapeDtypeStruct((comps, slots, points), F32)],
        [VMEM((slots * ROWS, points), F32)],
        [vmem] * 3,
    )(near(back.reshape(room, payload)), near(select), near(kernels))
    return fresh.reshape(velocity.shape), out.transpose(1, 0, 2)


def solution(mesh):
    return jax.shard_map(
        step,
        mesh=mesh,
        in_specs=(
            P(None, "gz", "gy", None),
            P(("gz", "gy"), None, None),
            P(("gz", "gy"), None, None),
            P(("gz", "gy"), None),
            P(("gz", "gy")),
            P(("gz", "gy")),
        ),
        out_specs=(P(None, "gz", "gy", None), P(("gz", "gy"), None, None)),
        check_vma=False,
    )
```

```python
import jax
import jax.numpy as jnp
from jax import lax
from jax.experimental import pallas as pl
from jax.experimental.pallas import tpu as pltpu
from jax.sharding import PartitionSpec as P


time_step = 0.25
viscosity = 0.5
F32 = jnp.float32
BF16 = jnp.bfloat16
LANES = 128
ROWS = 8
VMEM = pltpu.VMEM
TRANSPOSED = (((0,), (0,)), ((), ()))
NT = (((1,), (1,)), ((), ()))


def ring(count):
    half = count // 2
    return [count - 1 - (r % 2) * half - r // 2 for r in range(count)]


def seat(device, count):
    half = count // 2
    back = count - 1 - device
    return (back % half) * 2 + back // half


def iota(shape, axis):
    return lax.broadcasted_iota(jnp.int32, shape, axis)


def column(row):
    n = row.shape[1]
    same = iota((n, n), 0) == iota((n, n), 1)
    return jnp.sum(jnp.where(same, row, 0), axis=1, keepdims=True)


def dot(a, b, dims=(((1,), (0,)), ((), ()))):
    return lax.dot_general(a, b, dims, preferred_element_type=F32)


def spread(xblocks, counts, *refs):
    sources, (send, select, product, kernels), small, arrived = refs[:4], refs[4:8], refs[8:11], refs[11]
    forces, owners, blocks = small
    slots = kernels.shape[0]
    parts = arrived.shape[0] - len(small)
    tables = []
    for i, (source, target) in enumerate(zip(sources[1:], small)):
        tables.append(pltpu.make_async_copy(source, target, arrived.at[parts + i]))
        tables[-1].start()
    source = sources[0]
    each = slots // parts
    copies = []
    for i in range(parts):
        span = pl.ds(i * each, each)
        copies.append(pltpu.make_async_copy(source.at[span], kernels.at[span], arrived.at[i]))
        copies[-1].start()
    comps = forces.shape[0]
    cells = kernels.shape[2]
    room = send.shape[0] * send.shape[1]
    wide = select.shape[1]
    tall = slots * ROWS
    for copy in tables:
        copy.wait()
    owner_row = owners[...]
    owner = column(owner_row)
    block = column(blocks[...])
    here = iota((slots, slots), 0)
    there = iota((slots, slots), 1)
    earlier = (owner == owner_row) & (there < here)
    rank = jnp.sum(earlier.astype(jnp.int32), axis=1, keepdims=True)
    live = iota((slots, 1), 0) < counts[0]
    slot = jnp.where(live, seat(owner, room // 2) * 2 + rank, -1)
    choose = (slot == iota((slots, wide), 1)).astype(F32).astype(BF16)
    grow = (iota((tall, slots), 0) // ROWS == iota((tall, slots), 1)).astype(F32).astype(BF16)
    tall_choose = dot(grow, choose)
    select[...] = tall_choose.astype(BF16)
    grow_t = (iota((slots, tall), 1) // ROWS == iota((slots, tall), 0)).astype(F32).astype(BF16)
    wide_choose = dot(choose, grow_t, TRANSPOSED)
    flat = forces[...].reshape(comps * slots, forces.shape[2])
    r = iota((tall, comps * slots), 0)
    s = iota((tall, comps * slots), 1)
    order = ((r % ROWS) * slots + r // ROWS == s).astype(F32).astype(BF16)
    ordered = dot(order, flat)
    for p in range(slots):
        if p % each == 0:
            copies[p // each].wait()
        one = ordered[p * ROWS:(p + 1) * ROWS].astype(BF16)
        product[p * ROWS:(p + 1) * ROWS, :] = dot(one, kernels[p])
    made = product[...].astype(BF16)
    lane = iota(wide_choose.shape, 1) % ROWS
    for c in range(comps):
        pick = jnp.where(lane == c, wide_choose, 0.0).astype(BF16)
        send[:, :, c * cells:(c + 1) * cells] = dot(pick, made)[:room].reshape(room // 2, 2, cells).astype(BF16)
    where = iota((slots, LANES), 1)
    words = jnp.where(where == 0, block // xblocks, jnp.where(where == 1, block % xblocks, jnp.where(where == 2, 1, 0)))
    tags = dot(choose, words.astype(F32).astype(BF16), TRANSPOSED)
    send[:, :, comps * cells:] = tags[:room].reshape(room // 2, 2, LANES).astype(BF16)


def even(axis):
    return lax.axis_index(axis) % 2 == 0


def faces(planes, velocity, z_near, z_far, y_near, y_far, lifts):
    comps, height, _ = velocity.shape
    rows = height // planes
    z_even, y_even = even("gz"), even("gy")
    for c in range(comps):
        low, high = velocity[c, :rows, :].astype(BF16), velocity[c, height - rows:, :].astype(BF16)
        z_near[c] = jnp.where(z_even, high, low)
        z_far[c] = jnp.where(z_even, low, high)
        first, last = [jnp.concatenate([velocity[c, k * rows + row:k * rows + row + 1, :] for k in range(planes)], axis=0) for row in (0, rows - 1)]
        if c == 1:
            lifts[0] = viscosity + 0.5 * first
            lifts[1] = viscosity - 0.5 * last
        low, high = first.astype(BF16), last.astype(BF16)
        y_near[c] = jnp.where(y_even, high, low)
        y_far[c] = jnp.where(y_even, low, high)


def stencil(planes, velocity, base):
    comps, height, xcells = velocity.shape
    rows = height // planes
    x = iota((rows, xcells), 1)
    y = iota((rows, xcells), 0)
    for k in range(planes):
        span = slice(k * rows, (k + 1) * rows)
        center = [velocity[c, span, :] for c in range(comps)]
        for c in range(comps):
            v = center[c]
            x_up = jnp.where(x == xcells - 1, 0.0, pltpu.roll(v, xcells - 1, 1))
            x_down = jnp.where(x == 0, 0.0, pltpu.roll(v, 1, 1))
            y_up = jnp.where(y == rows - 1, 0.0, pltpu.roll(v, rows - 1, 0))
            y_down = jnp.where(y == 0, 0.0, pltpu.roll(v, 1, 0))
            z_up = velocity[c, (k + 1) * rows:(k + 2) * rows, :] if k + 1 < planes else 0.0
            z_down = velocity[c, (k - 1) * rows:k * rows, :] if k > 0 else 0.0
            lap = x_up + x_down + y_up + y_down + z_up + z_down - 6.0 * v
            adv = (center[0] * (x_up - x_down) + center[1] * (y_up - y_down) + center[2] * (z_up - z_down)) * 0.5
            base[c, span, :] = v + time_step * (viscosity * lap - adv)


def exchange(cells, planes, got, base, velocity, lifts, y_near, y_far, z_near, z_far, fresh, send):
    comps, height, xcells = base.shape
    rows = height // planes
    room = got.shape[0]
    xblocks = xcells // cells
    y_even, z_even = even("gy"), even("gz")
    tags = got[:, comps * cells:].astype(F32)
    row, xb, valid = tags[:, 0:1], tags[:, 1:2], tags[:, 2:3]
    at = iota((room, height), 1).astype(F32)
    match = (row == at) & (valid == 1.0)
    picks = [jnp.where(match & (xb == float(b)), 1.0, 0.0) for b in range(xblocks)]
    narrow = [p.astype(BF16) for p in picks]
    edge = iota((4 * planes, height), 0) % (2 * planes)
    spot = (edge % planes) * rows + jnp.where(edge >= planes, rows - 1, 0)
    edges = jnp.where(iota((4 * planes, height), 1) == spot, 1.0, 0.0)
    turned = [jnp.concatenate([p, edges], axis=0).T.astype(BF16) for p in picks]
    lift = velocity[comps - 1, :rows, :] * (0.5 * time_step) + viscosity * time_step
    sink = viscosity * time_step - velocity[comps - 1, height - rows:, :] * (0.5 * time_step)
    for c in range(comps):
        one, two = z_near[c].astype(F32), z_far[c].astype(F32)
        low = jnp.where(z_even, two, one) * lift
        high = jnp.where(z_even, one, two) * sink
        one, two = y_near[c].astype(F32), y_far[c].astype(F32)
        sides = jnp.concatenate([jnp.where(y_even, two, one) * lifts[0], jnp.where(y_even, one, two) * lifts[1]], axis=0)
        coarse = sides.astype(BF16)
        fine = (sides - coarse.astype(F32)).astype(BF16)
        total = None
        for b in range(xblocks):
            lanes = slice(b * cells, (b + 1) * cells)
            block = jnp.concatenate([got[:, c * cells:(c + 1) * cells], coarse[:, lanes], fine[:, lanes]], axis=0)
            flow = jnp.concatenate([low[:, lanes] + base[c, :rows, lanes], base[c, rows:height - rows, lanes], high[:, lanes] + base[c, height - rows:, lanes]], axis=0)
            new = flow + time_step * dot(turned[b], block)
            fresh[c, :, lanes] = new
            part = dot(narrow[b], new.astype(BF16))
            total = part if total is None else total + part
        send[:, :, c * cells:(c + 1) * cells] = total.reshape(send.shape[0], 2, cells).astype(BF16)


def sample(back, select, kernels, out, result):
    slots = kernels.shape[0]
    cells = kernels.shape[2]
    comps = out.shape[0]
    room = back.shape[0]
    chosen = select[:, :room].astype(F32)
    row = iota(chosen.shape, 0) % ROWS
    total = None
    for c in range(comps):
        pick = jnp.where(row == c, chosen, 0.0).astype(BF16)
        part = dot(pick, back[:, c * cells:(c + 1) * cells])
        total = part if total is None else total + part
    for p in range(slots):
        one = total[p * ROWS:(p + 1) * ROWS].astype(BF16)
        result[p * ROWS:(p + 1) * ROWS, :] = dot(one, kernels[p], NT)
    for c in range(comps):
        out[c] = result[pl.ds(c, slots, stride=ROWS), :]


def call(body, outs, scratch, ins, aliases={}):
    return pl.pallas_call(
        body,
        out_shape=outs,
        in_specs=ins,
        out_specs=[pl.BlockSpec(memory_space=VMEM)] * len(outs),
        scratch_shapes=scratch,
        input_output_aliases=aliases,
        compiler_params=pltpu.CompilerParams(vmem_limit_bytes=16 * 1024 * 1024),
    )


def pairs(count, first):
    low = range(first, count - 1, 2)
    return [(i, i + 1) for i in low] + [(i + 1, i) for i in low]


def near(x):
    return pltpu.with_memory_space_constraint(x, VMEM)


def step(velocity, forces, kernels, owners, blocks, counts):
    width_gy = lax.axis_size("gy")
    width_gz = lax.axis_size("gz")
    slots, comps, points = forces.shape
    cells = kernels.shape[2]
    planes, rows, xcells = velocity.shape[1:]
    xblocks = xcells // cells
    room = width_gy * 2
    wide = -(-room // LANES) * LANES
    payload = comps * cells
    parts = 4
    S = VMEM
    vmem = pl.BlockSpec(memory_space=VMEM)
    far = pl.BlockSpec(memory_space=pltpu.HBM)
    grid = near(velocity.reshape(comps, planes * rows, xcells))

    send, select = call(
        lambda *refs: spread(xblocks, *refs),
        [S((width_gy, 2, payload + LANES), BF16), S((slots * ROWS, wide), BF16)],
        [VMEM((slots * ROWS, cells), F32), VMEM(kernels.shape, BF16), VMEM((comps, slots, points), BF16), VMEM((1, slots), jnp.int32), VMEM((1, slots), jnp.int32), pltpu.SemaphoreType.DMA((parts + 3,))],
        [pl.BlockSpec(memory_space=pltpu.SMEM)] + [far] * 4,
    )(counts, *[pltpu.with_memory_space_constraint(x, pltpu.HBM) for x in (kernels, forces.transpose(1, 0, 2), owners.reshape(1, slots), blocks.reshape(1, slots))])
    got = lax.all_to_all(send, "gy", split_axis=0, concat_axis=0, tiled=True, axis_index_groups=[ring(width_gy)])
    got = got.reshape(room, payload + LANES)

    z_near, z_far, y_near, y_far, lifts = call(
        lambda *refs: faces(planes, *refs),
        [S((comps, rows, xcells), BF16)] * 2 + [S((comps, planes, xcells), BF16)] * 2 + [S((2, planes, xcells), F32)],
        [],
        [vmem],
    )(grid)
    y_near = lax.ppermute(y_near, "gy", pairs(width_gy, 0))
    y_far = lax.ppermute(y_far, "gy", pairs(width_gy, 1))
    z_near = lax.ppermute(z_near, "gz", pairs(width_gz, 0))
    z_far = lax.ppermute(z_far, "gz", pairs(width_gz, 1))
    (base,) = call(
        lambda *refs: stencil(planes, *refs),
        [S(grid.shape, F32)],
        [],
        [vmem],
    )(grid)

    fresh, picked = call(
        lambda *refs: exchange(cells, planes, *refs),
        [S(grid.shape, F32), S((width_gy, 2, payload), BF16)],
        [],
        [vmem] * 8,
        {1: 0},
    )(near(got), near(base), grid, near(lifts), near(y_near), near(y_far), near(z_near), near(z_far))
    back = lax.all_to_all(picked, "gy", split_axis=0, concat_axis=0, tiled=True, axis_index_groups=[ring(width_gy)])

    (out,) = call(
        sample,
        [jax.ShapeDtypeStruct((comps, slots, points), F32)],
        [VMEM((slots * ROWS, points), F32)],
        [vmem] * 3,
    )(near(back.reshape(room, payload)), near(select), near(kernels))
    return fresh.reshape(velocity.shape), out.transpose(1, 0, 2)


def solution(mesh):
    return jax.shard_map(
        step,
        mesh=mesh,
        in_specs=(
            P(None, "gz", "gy", None),
            P(("gz", "gy"), None, None),
            P(("gz", "gy"), None, None),
            P(("gz", "gy"), None),
            P(("gz", "gy")),
            P(("gz", "gy")),
        ),
        out_specs=(P(None, "gz", "gy", None), P(("gz", "gy"), None, None)),
        check_vma=False,
    )
```

```python
import jax
import jax.numpy as jnp
from jax import lax
from jax.experimental import pallas as pl
from jax.experimental.pallas import tpu as pltpu
from jax.sharding import PartitionSpec as P


time_step = 0.25
viscosity = 0.5
F32 = jnp.float32
BF16 = jnp.bfloat16
LANES = 128
ROWS = 8
VMEM = pltpu.VMEM
TRANSPOSED = (((0,), (0,)), ((), ()))
NT = (((1,), (1,)), ((), ()))


def ring(count):
    half = count // 2
    return [count - 1 - (r % 2) * half - r // 2 for r in range(count)]


def seat(device, count):
    half = count // 2
    back = count - 1 - device
    return (back % half) * 2 + back // half


def iota(shape, axis):
    return lax.broadcasted_iota(jnp.int32, shape, axis)


def column(row):
    n = row.shape[1]
    same = iota((n, n), 0) == iota((n, n), 1)
    return jnp.sum(jnp.where(same, row, 0), axis=1, keepdims=True)


def dot(a, b, dims=(((1,), (0,)), ((), ()))):
    return lax.dot_general(a, b, dims, preferred_element_type=F32)


def spread(xblocks, counts, *refs):
    sources, (outbox, select, product, kernels), small, arrived, send, sent = refs[:4], refs[4:8], refs[8:11], refs[11], refs[12], refs[13]
    leaving = []

    def leave(start, size):
        span = pl.ds(start, size)
        leaving.append(pltpu.make_async_copy(send.at[:, :, span], outbox.at[:, :, span], sent.at[len(leaving)]))
        leaving[-1].start()

    forces, owners, blocks = small
    slots = kernels.shape[0]
    parts = arrived.shape[0] - len(small)
    tables = []
    for i, (source, target) in enumerate(zip(sources[1:], small)):
        tables.append(pltpu.make_async_copy(source, target, arrived.at[parts + i]))
        tables[-1].start()
    source = sources[0]
    each = slots // parts
    copies = []
    for i in range(parts):
        span = pl.ds(i * each, each)
        copies.append(pltpu.make_async_copy(source.at[span], kernels.at[span], arrived.at[i]))
        copies[-1].start(priority=i % 2)
    comps = forces.shape[0]
    cells = kernels.shape[2]
    room = send.shape[0] * send.shape[1]
    wide = select.shape[1]
    tall = slots * ROWS
    for copy in tables:
        copy.wait()
    owner_row = owners[...]
    owner = column(owner_row)
    block = column(blocks[...])
    here = iota((slots, slots), 0)
    there = iota((slots, slots), 1)
    earlier = (owner == owner_row) & (there < here)
    rank = jnp.sum(earlier.astype(jnp.int32), axis=1, keepdims=True)
    live = iota((slots, 1), 0) < counts[0]
    slot = jnp.where(live, seat(owner, room // 2) * 2 + rank, -1)
    choose = (slot == iota((slots, wide), 1)).astype(F32).astype(BF16)
    grow = (iota((tall, slots), 0) // ROWS == iota((tall, slots), 1)).astype(F32).astype(BF16)
    tall_choose = dot(grow, choose)
    select[...] = tall_choose.astype(BF16)
    grow_t = (iota((slots, tall), 1) // ROWS == iota((slots, tall), 0)).astype(F32).astype(BF16)
    wide_choose = dot(choose, grow_t, TRANSPOSED)
    where = iota((slots, LANES), 1)
    words = jnp.where(where == 0, block // xblocks, jnp.where(where == 1, block % xblocks, jnp.where(where == 2, 1, 0)))
    tags = dot(choose, words.astype(F32).astype(BF16), TRANSPOSED)
    send[:, :, comps * cells:] = tags[:room].reshape(room // 2, 2, LANES).astype(BF16)
    leave(comps * cells, LANES)
    flat = forces[...].reshape(comps * slots, forces.shape[2])
    r = iota((tall, comps * slots), 0)
    s = iota((tall, comps * slots), 1)
    order = ((r % ROWS) * slots + r // ROWS == s).astype(F32).astype(BF16)
    ordered = dot(order, flat)
    for p in range(slots):
        if p % each == 0:
            copies[p // each].wait()
        one = ordered[p * ROWS:(p + 1) * ROWS].astype(BF16)
        product[p * ROWS:(p + 1) * ROWS, :] = dot(one, kernels[p])
    made = product[...].astype(BF16)
    lane = iota(wide_choose.shape, 1) % ROWS
    for c in range(comps):
        pick = jnp.where(lane == c, wide_choose, 0.0).astype(BF16)
        send[:, :, c * cells:(c + 1) * cells] = dot(pick, made)[:room].reshape(room // 2, 2, cells).astype(BF16)
        leave(c * cells, cells)
    for copy in leaving:
        copy.wait()


def even(axis):
    return lax.axis_index(axis) % 2 == 0


def faces(planes, velocity, z_near, z_far, y_near, y_far, lifts):
    comps, height, _ = velocity.shape
    rows = height // planes
    z_even, y_even = even("gz"), even("gy")
    for c in range(comps):
        low, high = velocity[c, :rows, :].astype(BF16), velocity[c, height - rows:, :].astype(BF16)
        z_near[c] = jnp.where(z_even, high, low)
        z_far[c] = jnp.where(z_even, low, high)
        first, last = [jnp.concatenate([velocity[c, k * rows + row:k * rows + row + 1, :] for k in range(planes)], axis=0) for row in (0, rows - 1)]
        if c == 1:
            lifts[0] = viscosity + 0.5 * first
            lifts[1] = viscosity - 0.5 * last
        low, high = first.astype(BF16), last.astype(BF16)
        y_near[c] = jnp.where(y_even, high, low)
        y_far[c] = jnp.where(y_even, low, high)


def stencil(planes, velocity, base):
    comps, height, xcells = velocity.shape
    rows = height // planes
    x = iota((rows, xcells), 1)
    y = iota((rows, xcells), 0)
    for k in range(planes):
        span = slice(k * rows, (k + 1) * rows)
        center = [velocity[c, span, :] for c in range(comps)]
        for c in range(comps):
            v = center[c]
            x_up = jnp.where(x == xcells - 1, 0.0, pltpu.roll(v, xcells - 1, 1))
            x_down = jnp.where(x == 0, 0.0, pltpu.roll(v, 1, 1))
            y_up = jnp.where(y == rows - 1, 0.0, pltpu.roll(v, rows - 1, 0))
            y_down = jnp.where(y == 0, 0.0, pltpu.roll(v, 1, 0))
            z_up = velocity[c, (k + 1) * rows:(k + 2) * rows, :] if k + 1 < planes else 0.0
            z_down = velocity[c, (k - 1) * rows:k * rows, :] if k > 0 else 0.0
            lap = x_up + x_down + y_up + y_down + z_up + z_down - 6.0 * v
            adv = (center[0] * (x_up - x_down) + center[1] * (y_up - y_down) + center[2] * (z_up - z_down)) * 0.5
            base[c, span, :] = v + time_step * (viscosity * lap - adv)


def exchange(cells, planes, got, base, velocity, lifts, y_near, y_far, z_near, z_far, fresh, target, send, sent):
    comps, height, xcells = base.shape
    rows = height // planes
    room = got.shape[0]
    xblocks = xcells // cells
    y_even, z_even = even("gy"), even("gz")
    tags = got[:, comps * cells:].astype(F32)
    row, xb, valid = tags[:, 0:1], tags[:, 1:2], tags[:, 2:3]
    at = iota((room, height), 1).astype(F32)
    match = (row == at) & (valid == 1.0)
    picks = [jnp.where(match & (xb == float(b)), 1.0, 0.0) for b in range(xblocks)]
    narrow = [p.astype(BF16) for p in picks]
    edge = iota((4 * planes, height), 0) % (2 * planes)
    spot = (edge % planes) * rows + jnp.where(edge >= planes, rows - 1, 0)
    edges = jnp.where(iota((4 * planes, height), 1) == spot, 1.0, 0.0)
    turned = [jnp.concatenate([p, edges], axis=0).T.astype(BF16) for p in picks]
    lift = velocity[comps - 1, :rows, :] * (0.5 * time_step) + viscosity * time_step
    sink = viscosity * time_step - velocity[comps - 1, height - rows:, :] * (0.5 * time_step)
    leaving = []
    for c in range(comps):
        one, two = z_near[c].astype(F32), z_far[c].astype(F32)
        low = jnp.where(z_even, two, one) * lift
        high = jnp.where(z_even, one, two) * sink
        one, two = y_near[c].astype(F32), y_far[c].astype(F32)
        sides = jnp.concatenate([jnp.where(y_even, two, one) * lifts[0], jnp.where(y_even, one, two) * lifts[1]], axis=0)
        coarse = sides.astype(BF16)
        fine = (sides - coarse.astype(F32)).astype(BF16)
        total = None
        for b in range(xblocks):
            lanes = slice(b * cells, (b + 1) * cells)
            block = jnp.concatenate([got[:, c * cells:(c + 1) * cells], coarse[:, lanes], fine[:, lanes]], axis=0)
            flow = jnp.concatenate([low[:, lanes] + base[c, :rows, lanes], base[c, rows:height - rows, lanes], high[:, lanes] + base[c, height - rows:, lanes]], axis=0)
            new = flow + time_step * dot(turned[b], block)
            fresh[c, :, lanes] = new
            part = dot(narrow[b], new.astype(BF16))
            total = part if total is None else total + part
        span = pl.ds(c * cells, cells)
        send[:, :, span] = total.reshape(send.shape[0], 2, cells).astype(BF16)
        leaving.append(pltpu.make_async_copy(send.at[:, :, span], target.at[:, :, span], sent.at[c]))
        leaving[-1].start()
    for copy in leaving:
        copy.wait()


def sample(back, select, kernels, out, result):
    slots = kernels.shape[0]
    cells = kernels.shape[2]
    comps = out.shape[0]
    room = back.shape[0]
    chosen = select[:, :room].astype(F32)
    row = iota(chosen.shape, 0) % ROWS
    total = None
    for c in range(comps):
        pick = jnp.where(row == c, chosen, 0.0).astype(BF16)
        part = dot(pick, back[:, c * cells:(c + 1) * cells])
        total = part if total is None else total + part
    for p in range(slots):
        one = total[p * ROWS:(p + 1) * ROWS].astype(BF16)
        result[p * ROWS:(p + 1) * ROWS, :] = dot(one, kernels[p], NT)
    for c in range(comps):
        out[c] = result[pl.ds(c, slots, stride=ROWS), :]


def call(body, outs, scratch, ins, aliases={}, places=None):
    return pl.pallas_call(
        body,
        out_shape=outs,
        in_specs=ins,
        out_specs=places or [pl.BlockSpec(memory_space=VMEM)] * len(outs),
        scratch_shapes=scratch,
        input_output_aliases=aliases,
        compiler_params=pltpu.CompilerParams(vmem_limit_bytes=16 * 1024 * 1024),
    )


def pairs(count, first):
    low = range(first, count - 1, 2)
    return [(i, i + 1) for i in low] + [(i + 1, i) for i in low]


def near(x):
    return pltpu.with_memory_space_constraint(x, VMEM)


def step(velocity, forces, kernels, owners, blocks, counts):
    width_gy = lax.axis_size("gy")
    width_gz = lax.axis_size("gz")
    slots, comps, points = forces.shape
    cells = kernels.shape[2]
    planes, rows, xcells = velocity.shape[1:]
    xblocks = xcells // cells
    room = width_gy * 2
    wide = -(-room // LANES) * LANES
    payload = comps * cells
    parts = 4
    S = VMEM
    vmem = pl.BlockSpec(memory_space=VMEM)
    far = pl.BlockSpec(memory_space=pltpu.HBM)
    grid = near(velocity.reshape(comps, planes * rows, xcells))

    send, select = call(
        lambda *refs: spread(xblocks, *refs),
        [jax.ShapeDtypeStruct((width_gy, 2, payload + LANES), BF16), S((slots * ROWS, wide), BF16)],
        [VMEM((slots * ROWS, cells), F32), VMEM(kernels.shape, BF16), VMEM((comps, slots, points), BF16), VMEM((1, slots), jnp.int32), VMEM((1, slots), jnp.int32), pltpu.SemaphoreType.DMA((parts + 3,)), VMEM((width_gy, 2, payload + LANES), BF16), pltpu.SemaphoreType.DMA((comps + 1,))],
        [pl.BlockSpec(memory_space=pltpu.SMEM)] + [far] * 4,
        places=[far, vmem],
    )(counts, *[pltpu.with_memory_space_constraint(x, pltpu.HBM) for x in (kernels, forces.transpose(1, 0, 2), owners.reshape(1, slots), blocks.reshape(1, slots))])
    got = lax.all_to_all(send, "gy", split_axis=0, concat_axis=0, tiled=True, axis_index_groups=[ring(width_gy)])
    got = got.reshape(room, payload + LANES)

    z_near, z_far, y_near, y_far, lifts = call(
        lambda *refs: faces(planes, *refs),
        [S((comps, rows, xcells), BF16)] * 2 + [S((comps, planes, xcells), BF16)] * 2 + [S((2, planes, xcells), F32)],
        [],
        [vmem],
    )(grid)
    y_near = lax.ppermute(y_near, "gy", pairs(width_gy, 0))
    y_far = lax.ppermute(y_far, "gy", pairs(width_gy, 1))
    z_near = lax.ppermute(z_near, "gz", pairs(width_gz, 0))
    z_far = lax.ppermute(z_far, "gz", pairs(width_gz, 1))
    (base,) = call(
        lambda *refs: stencil(planes, *refs),
        [S(grid.shape, F32)],
        [],
        [vmem],
    )(grid)

    fresh, picked = call(
        lambda *refs: exchange(cells, planes, *refs),
        [S(grid.shape, F32), jax.ShapeDtypeStruct((width_gy, 2, payload), BF16)],
        [VMEM((width_gy, 2, payload), BF16), pltpu.SemaphoreType.DMA((comps,))],
        [vmem] * 8,
        {1: 0},
        [vmem, far],
    )(near(got), near(base), grid, near(lifts), near(y_near), near(y_far), near(z_near), near(z_far))
    back = lax.all_to_all(picked, "gy", split_axis=0, concat_axis=0, tiled=True, axis_index_groups=[ring(width_gy)])

    (out,) = call(
        sample,
        [jax.ShapeDtypeStruct((comps, slots, points), F32)],
        [VMEM((slots * ROWS, points), F32)],
        [vmem] * 3,
    )(near(back.reshape(room, payload)), near(select), near(kernels))
    return fresh.reshape(velocity.shape), out.transpose(1, 0, 2)


def solution(mesh):
    return jax.shard_map(
        step,
        mesh=mesh,
        in_specs=(
            P(None, "gz", "gy", None),
            P(("gz", "gy"), None, None),
            P(("gz", "gy"), None, None),
            P(("gz", "gy"), None),
            P(("gz", "gy")),
            P(("gz", "gy")),
        ),
        out_specs=(P(None, "gz", "gy", None), P(("gz", "gy"), None, None)),
        check_vma=False,
    )
```
